32 devices in a mesh: rows: 8 (over z, y), pairs: 4 (over x, core).
Axes of the slice: x: 2, y: 2, z: 4, core: 2. Of those that a mesh axis runs over, the one named last changes fastest.
Arguments:
- matrix: float32 [16384, 2048], P('rows', 'pairs'), may hold values from -40 to 40
Outputs:
- rotated: float32 [16384, 2048], P('rows', 'pairs')
The draws below stay inside these ranges and needn't reach their ends.
All inputs are finite; a program needn't handle non-finite values.
Results may differ from the reference program's by a relative error of at most 0.0001.
Values sent between devices are 32-bit elements; how exact they have to be, the bound alone decides.
A program may use at most 64 MiB of HBM per device.

```python
import jax
import jax.numpy as jnp
from jax import lax

B = 256
STEPS = 2
PAIRS = 4
ROWS = 16384
COLS = 2048


def draw_matrix(key, part):
    keys = jax.random.split(jax.random.fold_in(key, 17), 4)
    independent = jax.random.normal(keys[0], (ROWS, COLS), jnp.float32)
    shared_scale = 0.05
    factors = jax.random.normal(keys[1], (ROWS, 64), jnp.float32)
    loadings = jax.random.normal(keys[2], (64, COLS), jnp.float32) * shared_scale
    shared = jnp.dot(factors, loadings, preferred_element_type=jnp.float32)
    col_scale = jnp.exp(jax.random.uniform(keys[3], (1, COLS), jnp.float32, jnp.log(0.3), jnp.log(3.0)))
    values = (independent + shared) * col_scale
    return jnp.clip(values, -40.0, 40.0).astype(jnp.float32)


def setup_inputs(seed: int = 0) -> dict:
    key_list = jax.random.split(jax.random.key(seed), 2)
    matrix = draw_matrix(jax.random.fold_in(key_list[1], 71), 0)
    return dict(matrix=matrix)


def spd_solve(system, right_side):
    factor = jnp.linalg.cholesky(system)
    middle = lax.linalg.triangular_solve(factor, right_side, left_side=True, lower=True)
    return lax.linalg.triangular_solve(factor, middle, left_side=True, lower=True, transpose_a=True)

def cayley_rotation(cross_block, norms_first, norms_second, rows_all):
    precise = lax.Precision.HIGHEST
    block_cols = cross_block.shape[0]
    scale_first = lax.rsqrt(norms_first / rows_all + 1e-06)
    scale_second = lax.rsqrt(norms_second / rows_all + 1e-06)
    coupling = 0.5 * cross_block * scale_first[:, None] * scale_second[None, :] / rows_all
    identity = jnp.eye(block_cols, dtype=jnp.float32)
    first_system = identity + jnp.dot(coupling.astype(jnp.float32), coupling.T.astype(jnp.float32), precision=precise, preferred_element_type=jnp.float32)
    first_sol = spd_solve(first_system, jnp.concatenate([identity, coupling], axis=1))
    lower_sol = jnp.dot(coupling.T.astype(jnp.float32), first_sol.astype(jnp.float32), precision=precise, preferred_element_type=jnp.float32)
    upper_rows = jnp.concatenate([2.0 * first_sol[:, :block_cols] - identity, 2.0 * first_sol[:, block_cols:]], axis=1)
    lower_rows = jnp.concatenate([-2.0 * lower_sol[:, :block_cols], identity - 2.0 * lower_sol[:, block_cols:]], axis=1)
    return jnp.concatenate([upper_rows, lower_rows], axis=0)

def reference(matrix):
    precise = lax.Precision.HIGHEST
    grouped = matrix.reshape(ROWS, PAIRS, 2, B)
    first_blocks = jnp.transpose(grouped[:, :, 0, :], (1, 0, 2))
    second_blocks = jnp.transpose(grouped[:, :, 1, :], (1, 0, 2))

    def turn_pair(pair_blocks):
        both = jnp.concatenate([pair_blocks[0], pair_blocks[1]], axis=1)
        gram_pair = lax.dot_general(both.astype(jnp.float32), both.astype(jnp.float32), (((0,), (0,)), ((), ())), precision=precise, preferred_element_type=jnp.float32)
        diag_all = jnp.diagonal(gram_pair)
        rotate = cayley_rotation(gram_pair[:B, B:], diag_all[:B], diag_all[B:], ROWS)
        turned = jnp.dot(both.astype(jnp.float32), rotate.astype(jnp.float32), precision=precise, preferred_element_type=jnp.float32)
        return (turned[:, :B], turned[:, B:])
    for turn_index in range(STEPS):
        first_blocks, second_blocks = lax.map(turn_pair, (first_blocks, second_blocks))
        next_first = jnp.concatenate([first_blocks[:1], second_blocks[:1], first_blocks[1:-1]], axis=0)
        second_blocks = jnp.concatenate([second_blocks[1:], first_blocks[-1:]], axis=0)
        first_blocks = next_first
    stacked = jnp.stack([first_blocks, second_blocks], axis=2)
    return jnp.transpose(stacked, (1, 0, 2, 3)).reshape(ROWS, COLS)
```

```python
import functools

import jax
import jax.numpy as jnp
from jax import lax
from jax.experimental import pallas as pl
from jax.experimental.pallas import tpu as pltpu
from jax.sharding import PartitionSpec as P

STEPS = 2
CHUNKS = 8
F32 = jnp.float32
BF16 = jnp.bfloat16
MESH = pl.DeviceIdType.MESH


def split(value):
    high = value.astype(BF16)
    return high, (value - high.astype(F32)).astype(BF16)


def dot_bf16(left, right, left_dim):
    return lax.dot_general(
        left, right, (((left_dim,), (0,)), ((), ())), preferred_element_type=F32
    )


def dot_three(left, right, left_dim):
    return (
        dot_bf16(left[0], right[1], left_dim)
        + dot_bf16(left[1], right[0], left_dim)
        + dot_bf16(left[0], right[0], left_dim)
    )


def exact_dot(left, right, left_dim=1):
    return lax.dot_general(
        left,
        right,
        (((left_dim,), (0,)), ((), ())),
        precision=lax.Precision.HIGHEST,
        preferred_element_type=F32,
    )


def sum_over_rows(count, part, total, recv, mine, gathered, sems):
    send_one, recv_one, send_two, recv_two = sems
    me = lax.axis_index("rows")
    first_copies = []
    for far in range(1, count):
        peer = lax.rem(me + far, count)
        copy = pltpu.make_async_remote_copy(
            src_ref=part.at[peer],
            dst_ref=recv.at[far],
            send_sem=send_one.at[far],
            recv_sem=recv_one.at[far],
            device_id={"rows": peer},
            device_id_type=MESH,
        )
        copy.start()
        first_copies.append(copy)
    acc = part[me]
    for far in range(1, count):
        first_copies[far - 1].wait_recv()
        acc = acc + recv[far]
    mine[...] = acc
    second_copies = []
    for far in range(1, count):
        peer = lax.rem(me + far, count)
        copy = pltpu.make_async_remote_copy(
            src_ref=mine,
            dst_ref=gathered.at[far],
            send_sem=send_two.at[far],
            recv_sem=recv_two.at[far],
            device_id={"rows": peer},
            device_id_type=MESH,
        )
        copy.start()
        second_copies.append(copy)
    total[me] = acc
    for far in range(1, count):
        second_copies[far - 1].wait_recv()
        total[lax.rem(me + count - far, count)] = gathered[far]
    for copy in first_copies + second_copies:
        copy.wait_send()


def stage_kernel(rotates, sums, count, length, *refs):
    refs = list(refs)
    matrix = refs.pop(0)
    if rotates:
        rot_high, rot_low = refs.pop(0), refs.pop(0)
        moved = refs.pop(0)
    if sums:
        total = refs.pop(0)
    loaded, load_sem = refs.pop(0), refs.pop(0)
    if rotates:
        up, other, land_first, land_second = (refs.pop(0) for _ in range(4))
        up_send, up_recv, down_send, down_recv, store_sem = (refs.pop(0) for _ in range(5))
    if sums:
        cross, norms, part, recv, mine, gathered = (refs.pop(0) for _ in range(6))
        sums_sems = tuple(refs.pop(0) for _ in range(4))
    rows, cols = loaded.shape
    block = cols // 2
    step = rows // CHUNKS
    position = lax.axis_index("pairs")
    lowest = position == 0
    highest = position == length - 1

    def at(chunk):
        return pl.ds(pl.multiple_of(chunk * step, step), step)

    def load(chunk):
        return pltpu.make_async_copy(
            matrix.at[at(chunk)], loaded.at[at(chunk)], load_sem.at[chunk]
        )

    def to_upper(chunk):
        return pltpu.make_async_remote_copy(
            src_ref=up.at[at(chunk)],
            dst_ref=land_first.at[at(chunk)],
            send_sem=up_send.at[chunk],
            recv_sem=up_recv.at[chunk],
            device_id={"pairs": lax.rem(position + 1, length)},
            device_id_type=MESH,
        )

    def to_lower(chunk):
        return pltpu.make_async_remote_copy(
            src_ref=other.at[at(chunk)],
            dst_ref=land_second.at[at(chunk)],
            send_sem=down_send.at[chunk],
            recv_sem=down_recv.at[chunk],
            device_id={"pairs": lax.rem(position + length - 1, length)},
            device_id_type=MESH,
        )

    def store(chunk, half):
        source = land_second if half else land_first
        return pltpu.make_async_copy(
            source.at[at(chunk)],
            moved.at[at(chunk), pl.ds(half * block, block)],
            store_sem.at[half, chunk],
        )

    for chunk in range(CHUNKS):
        load(chunk).start()

    barrier = pltpu.get_barrier_semaphore()
    if sums:
        me = lax.axis_index("rows")
        for far in range(1, count):
            pl.semaphore_signal(
                barrier,
                inc=1,
                device_id={"rows": lax.rem(me + far, count)},
                device_id_type=MESH,
            )
    greeted = jnp.int32(count - 1 if sums else 0)
    if rotates:
        @pl.when(jnp.logical_not(lowest))
        def _():
            pl.semaphore_signal(
                barrier, inc=1, device_id={"pairs": position - 1}, device_id_type=MESH
            )

        @pl.when(jnp.logical_not(highest))
        def _():
            pl.semaphore_signal(
                barrier, inc=1, device_id={"pairs": position + 1}, device_id_type=MESH
            )

        greeted = greeted + jnp.where(lowest, 0, 1) + jnp.where(highest, 0, 1)
    pl.semaphore_wait(barrier, greeted)

    if rotates:
        def turn(chunk, carry):
            load(chunk).wait()
            turned = dot_three(split(loaded[at(chunk), :]), (rot_high[...], rot_low[...]), 1)
            left, right = turned[:, :block], turned[:, block:]
            up[at(chunk), :] = jnp.where(lowest, right, left)
            other[at(chunk), :] = jnp.where(lowest, left, right)

            @pl.when(jnp.logical_not(highest))
            def _():
                to_upper(chunk).start()

            @pl.when(highest)
            def _():
                land_second[at(chunk), :] = left

            @pl.when(jnp.logical_not(lowest))
            def _():
                to_lower(chunk).start()

            @pl.when(lowest)
            def _():
                land_first[at(chunk), :] = left

            return carry

        lax.fori_loop(0, CHUNKS, turn, 0)

    if sums:
        cross[...] = jnp.zeros_like(cross)
        norms[...] = jnp.zeros_like(norms)

    def take(chunk, carry):
        if rotates:
            @pl.when(jnp.logical_not(lowest))
            def _():
                to_upper(chunk).wait_recv()

            @pl.when(jnp.logical_not(highest))
            def _():
                to_lower(chunk).wait_recv()

            store(chunk, 0).start()
            store(chunk, 1).start()
        else:
            load(chunk).wait()
        if sums:
            if rotates:
                first, second = land_first[at(chunk), :], land_second[at(chunk), :]
            else:
                first, second = loaded[at(chunk), :block], loaded[at(chunk), block:]
            cross[...] += dot_three(split(first), split(second), 0)
            norms[0:1, :] += jnp.sum(first * first, axis=0, keepdims=True)
            norms[1:2, :] += jnp.sum(second * second, axis=0, keepdims=True)
        return carry

    lax.fori_loop(0, CHUNKS, take, 0)

    if sums:
        share = block // count
        half = block // 2
        for slot in range(count):
            part[slot, :share, :] = cross[slot * share : (slot + 1) * share, :half]
            part[slot, share : 2 * share, :] = cross[slot * share : (slot + 1) * share, half:]
            part[slot, 2 * share : 2 * share + 8, :] = norms[:, :half]
            part[slot, 2 * share + 8 : 2 * share + 16, :] = norms[:, half:]
        sum_over_rows(count, part, total, recv, mine, gathered, sums_sems)

    if rotates:
        def finish(chunk, carry):
            @pl.when(jnp.logical_not(highest))
            def _():
                to_upper(chunk).wait_send()

            @pl.when(jnp.logical_not(lowest))
            def _():
                to_lower(chunk).wait_send()

            store(chunk, 0).wait()
            store(chunk, 1).wait()
            return carry

        lax.fori_loop(0, CHUNKS, finish, 0)


def stage(name, number, matrix, rotation, sums):
    rows, cols = matrix.shape
    block = cols // 2
    count = lax.axis_size("rows")
    length = lax.axis_size("pairs")
    rotates = rotation is not None
    slot = (2 * (block // count) + 16, block // 2)
    hbm = pl.BlockSpec(memory_space=pl.ANY)
    vmem = pl.BlockSpec(memory_space=pltpu.VMEM)
    dma = pltpu.SemaphoreType.DMA
    in_specs, outs, out_specs = [hbm], [], []
    scratch = [pltpu.VMEM((rows, cols), F32), dma((CHUNKS,))]
    if rotates:
        in_specs += [vmem, vmem]
        outs.append(jax.ShapeDtypeStruct((rows, cols), F32))
        out_specs.append(hbm)
        scratch += [pltpu.VMEM((rows, block), F32)] * 4
        scratch += [dma((CHUNKS,))] * 4 + [dma((2, CHUNKS))]
    if sums:
        outs.append(jax.ShapeDtypeStruct((count,) + slot, F32))
        out_specs.append(vmem)
        scratch += [pltpu.VMEM((block, block), F32), pltpu.VMEM((8, block), F32)]
        scratch += [pltpu.VMEM((count,) + slot, F32)] * 2 + [pltpu.VMEM(slot, F32)]
        scratch += [pltpu.VMEM((count,) + slot, F32)]
        scratch += [dma((count,))] * 4
    return pl.pallas_call(
        functools.partial(stage_kernel, rotates, sums, count, length),
        out_shape=outs,
        in_specs=in_specs,
        out_specs=out_specs,
        scratch_shapes=scratch,
        name=name,
        compiler_params=pltpu.CompilerParams(
            collective_id=number, has_side_effects=True, vmem_limit_bytes=50 * 2**20
        ),
    )(matrix, *(rotation or ()))


def rotation_kernel(rows_all, total, rot_high, rot_low, coupling, inverse, residual):
    count, depth, half = total.shape
    block = 2 * half
    share = (depth - 16) // 2
    for slot in range(count):
        coupling[slot * share : (slot + 1) * share, :half] = total[slot, :share, :]
        coupling[slot * share : (slot + 1) * share, half:] = total[slot, share : 2 * share, :]
    norms = jnp.concatenate(
        [total[0, 2 * share : 2 * share + 8, :], total[0, 2 * share + 8 :, :]], axis=1
    )
    scales = lax.rsqrt(norms / rows_all + 1e-06)
    row = lax.broadcasted_iota(jnp.int32, (block, block), 0)
    col = lax.broadcasted_iota(jnp.int32, (block, block), 1)
    identity = jnp.where(row == col, 1.0, 0.0).astype(F32)
    scale_first = jnp.sum(identity * scales[0:1, :], axis=1, keepdims=True)
    coupling[...] = 0.5 * coupling[...] * scale_first * scales[1:2, :] / rows_all
    turn = coupling[...]
    gram = lax.dot_general(
        turn,
        turn,
        (((1,), (1,)), ((), ())),
        precision=lax.Precision.HIGHEST,
        preferred_element_type=F32,
    )
    spread = jnp.max(jnp.sum(jnp.abs(gram), axis=1, keepdims=True))
    start = 2.0 / (2.0 + spread)
    first = (1.0 - start) * identity - start * gram
    inverse[...] = start * (identity + first)
    bound = spread / (2.0 + spread)
    residual[...] = exact_dot(first, first)

    def grow(state):
        limit, trips = state
        both = exact_dot(jnp.concatenate([inverse[...], residual[...]], axis=0), residual[...])
        inverse[...] += both[:block]
        residual[...] = both[block:]
        return limit * limit, trips + 1

    lax.while_loop(
        lambda state: jnp.logical_and(state[0] > 1e-07, state[1] < 30),
        grow,
        (bound * bound, jnp.int32(0)),
    )

    def correct(index, carry):
        guess = inverse[...]
        residual[...] = identity - guess - exact_dot(gram, guess)
        inverse[...] = guess + exact_dot(guess, residual[...])
        return carry

    lax.fori_loop(0, jnp.where(spread > 32.0, 4, 0), correct, 0)
    upper = exact_dot(inverse[...], turn)
    lower = exact_dot(turn, upper, 0)
    parts = (
        (0, 0, 2.0 * inverse[...] - identity),
        (0, 1, 2.0 * upper),
        (1, 0, -2.0 * upper.T),
        (1, 1, identity - 2.0 * lower),
    )
    for down, across, value in parts:
        high, low = split(value)
        where = (pl.ds(down * block, block), pl.ds(across * block, block))
        rot_high[where] = high
        rot_low[where] = low


def rotation_of(total, rows_all):
    block = 2 * total.shape[2]
    vmem = pl.BlockSpec(memory_space=pltpu.VMEM)
    return pl.pallas_call(
        functools.partial(rotation_kernel, rows_all),
        out_shape=[jax.ShapeDtypeStruct((2 * block, 2 * block), BF16)] * 2,
        in_specs=[vmem],
        out_specs=[vmem, vmem],
        scratch_shapes=[pltpu.VMEM((block, block), F32)] * 3,
        name="rotation",
        compiler_params=pltpu.CompilerParams(vmem_limit_bytes=32 * 2**20),
    )(total)


def shards(matrix):
    rows_all = matrix.shape[0] * lax.axis_size("rows")
    (total,) = stage("products", 0, matrix, None, True)
    for turn_index in range(STEPS - 1):
        rotation = rotation_of(total, rows_all)
        matrix, total = stage("turn_and_products", 1, matrix, rotation, True)
    rotation = rotation_of(total, rows_all)
    (matrix,) = stage("last_turn", 2, matrix, rotation, False)
    return matrix


def solution(mesh):
    return jax.shard_map(
        shards,
        mesh=mesh,
        in_specs=(P("rows", "pairs"),),
        out_specs=P("rows", "pairs"),
        check_vma=False,
    )
```

```python
import functools

import jax
import jax.numpy as jnp
from jax import lax
from jax.experimental import pallas as pl
from jax.experimental.pallas import tpu as pltpu
from jax.sharding import PartitionSpec as P

CHUNKS = 8
LATE = 2
F32 = jnp.float32
BF16 = jnp.bfloat16
MESH = pl.DeviceIdType.MESH


def split(value):
    high = value.astype(BF16)
    return high, (value - high.astype(F32)).astype(BF16)


def dot_bf16(left, right, left_dim):
    return lax.dot_general(
        left, right, (((left_dim,), (0,)), ((), ())), preferred_element_type=F32
    )


def dot_three(left, right, left_dim):
    return (
        dot_bf16(left[0], right[1], left_dim)
        + dot_bf16(left[1], right[0], left_dim)
        + dot_bf16(left[0], right[0], left_dim)
    )


def exact_dot(left, right, left_dim=1):
    return lax.dot_general(
        left,
        right,
        (((left_dim,), (0,)), ((), ())),
        precision=lax.Precision.HIGHEST,
        preferred_element_type=F32,
    )


def sum_over_rows(count, part, total, recv, mine, gathered, sems, beside):
    send_one, recv_one, send_two, recv_two = sems
    me = lax.axis_index("rows")
    first_copies = []
    for far in range(1, count):
        peer = lax.rem(me + far, count)
        copy = pltpu.make_async_remote_copy(
            src_ref=part.at[peer],
            dst_ref=recv.at[far],
            send_sem=send_one.at[far],
            recv_sem=recv_one.at[far],
            device_id={"rows": peer},
            device_id_type=MESH,
        )
        copy.start()
        first_copies.append(copy)
    acc = part[me]
    for far in range(1, count):
        first_copies[far - 1].wait_recv()
        acc = acc + recv[far]
    mine[...] = acc
    second_copies = []
    for far in range(1, count):
        peer = lax.rem(me + far, count)
        copy = pltpu.make_async_remote_copy(
            src_ref=mine,
            dst_ref=gathered.at[far],
            send_sem=send_two.at[far],
            recv_sem=recv_two.at[far],
            device_id={"rows": peer},
            device_id_type=MESH,
        )
        copy.start()
        second_copies.append(copy)
    if beside:
        partner, has_partner, total_near, gathered_near, send_near, recv_near = beside

        def to_near(far):
            return pltpu.make_async_remote_copy(
                src_ref=mine,
                dst_ref=gathered_near.at[far],
                send_sem=send_near.at[far],
                recv_sem=recv_near.at[far],
                device_id={"rows": lax.rem(me + far, count), "pairs": partner},
                device_id_type=MESH,
            )

        @pl.when(has_partner)
        def _():
            for far in range(count):
                to_near(far).start()

    total[me] = acc
    for far in range(1, count):
        second_copies[far - 1].wait_recv()
        total[lax.rem(me + count - far, count)] = gathered[far]
    if beside:
        @pl.when(has_partner)
        def _():
            for far in range(count):
                to_near(far).wait_recv()
                total_near[lax.rem(me + count - far, count)] = gathered_near[far]
            for far in range(count):
                to_near(far).wait_send()

        @pl.when(jnp.logical_not(has_partner))
        def _():
            total_near[...] = total[...]

    for copy in first_copies + second_copies:
        copy.wait_send()


def stage_kernel(rotates, sums, ahead, count, length, *refs):
    refs = list(refs)
    matrix = refs.pop(0)
    if rotates:
        rot_high, rot_low = refs.pop(0), refs.pop(0)
        if ahead and not sums:
            kept, extra, near_high, near_low = (refs.pop(0) for _ in range(4))
        moved = refs.pop(0)
    if sums:
        total = refs.pop(0)
        if ahead:
            kept, extra, total_near = (refs.pop(0) for _ in range(3))
    loaded, load_sem = refs.pop(0), refs.pop(0)
    if rotates:
        up, other, land_first, land_second = (refs.pop(0) for _ in range(4))
        up_send, up_recv, down_send, down_recv, store_sem = (refs.pop(0) for _ in range(5))
    if sums:
        cross, norms, part, recv, mine, gathered = (refs.pop(0) for _ in range(6))
        sums_sems = tuple(refs.pop(0) for _ in range(4))
    if ahead and sums:
        land_extra, gathered_near = refs.pop(0), refs.pop(0)
        extra_send, extra_recv, send_near, recv_near, side_sem = (refs.pop(0) for _ in range(5))
    if ahead and not sums:
        had_kept, had_extra, side_sem = (refs.pop(0) for _ in range(3))
    rows, cols = loaded.shape
    block = cols // 2
    step = rows // CHUNKS
    position = lax.axis_index("pairs")
    lowest = position == 0
    highest = position == length - 1
    odd = lax.rem(position, 2) == 1
    even = jnp.logical_not(odd)
    has_partner = jnp.logical_or(
        jnp.logical_and(odd, position < length - 1), jnp.logical_and(even, position > 0)
    )
    sends_extra = jnp.logical_or(
        jnp.logical_and(even, position + 2 < length), jnp.logical_and(odd, position >= 2)
    )
    gets_extra = jnp.logical_or(
        jnp.logical_and(even, position >= 2), jnp.logical_and(odd, position + 2 < length)
    )
    partner = lax.rem(position + jnp.where(odd, 1, length - 1), length)

    def at(chunk):
        return pl.ds(pl.multiple_of(chunk * step, step), step)

    def load(chunk):
        return pltpu.make_async_copy(
            matrix.at[at(chunk)], loaded.at[at(chunk)], load_sem.at[chunk]
        )

    def to_upper(chunk):
        return pltpu.make_async_remote_copy(
            src_ref=up.at[at(chunk)],
            dst_ref=land_first.at[at(chunk)],
            send_sem=up_send.at[chunk],
            recv_sem=up_recv.at[chunk],
            device_id={"pairs": lax.rem(position + 1, length)},
            device_id_type=MESH,
        )

    def to_lower(chunk):
        return pltpu.make_async_remote_copy(
            src_ref=other.at[at(chunk)],
            dst_ref=land_second.at[at(chunk)],
            send_sem=down_send.at[chunk],
            recv_sem=down_recv.at[chunk],
            device_id={"pairs": lax.rem(position + length - 1, length)},
            device_id_type=MESH,
        )

    def store(chunk, half):
        source = land_second if half else land_first
        return pltpu.make_async_copy(
            source.at[at(chunk)],
            moved.at[at(chunk), pl.ds(half * block, block)],
            store_sem.at[half, chunk],
        )

    def to_extra(chunk, source, target):
        return pltpu.make_async_remote_copy(
            src_ref=source.at[at(chunk)],
            dst_ref=land_extra.at[at(chunk)],
            send_sem=extra_send.at[chunk],
            recv_sem=extra_recv.at[chunk],
            device_id={"pairs": lax.rem(target + length, length)},
            device_id_type=MESH,
        )

    def keep(chunk, source):
        return pltpu.make_async_copy(source.at[at(chunk)], kept.at[at(chunk)], side_sem.at[0, chunk])

    def store_extra(chunk):
        return pltpu.make_async_copy(
            land_extra.at[at(chunk)], extra.at[at(chunk)], side_sem.at[1, chunk]
        )

    def load_side(chunk):
        return (
            pltpu.make_async_copy(kept.at[at(chunk)], had_kept.at[at(chunk)], side_sem.at[0, chunk]),
            pltpu.make_async_copy(extra.at[at(chunk)], had_extra.at[at(chunk)], side_sem.at[1, chunk]),
        )

    for chunk in range(CHUNKS):
        load(chunk).start()
        if ahead and not sums and chunk >= LATE:
            for copy in load_side(chunk):
                copy.start()

    barrier = pltpu.get_barrier_semaphore()
    if sums:
        me = lax.axis_index("rows")
        for far in range(1, count):
            pl.semaphore_signal(
                barrier,
                inc=1,
                device_id={"rows": lax.rem(me + far, count)},
                device_id_type=MESH,
            )
    greeted = jnp.int32(count - 1 if sums else 0)
    if rotates:
        @pl.when(jnp.logical_not(lowest))
        def _():
            pl.semaphore_signal(
                barrier, inc=1, device_id={"pairs": position - 1}, device_id_type=MESH
            )

        @pl.when(jnp.logical_not(highest))
        def _():
            pl.semaphore_signal(
                barrier, inc=1, device_id={"pairs": position + 1}, device_id_type=MESH
            )

        greeted = greeted + jnp.where(lowest, 0, 1) + jnp.where(highest, 0, 1)
    if ahead and sums:
        @pl.when(position >= 2)
        def _():
            pl.semaphore_signal(
                barrier, inc=1, device_id={"pairs": position - 2}, device_id_type=MESH
            )

        @pl.when(position + 2 < length)
        def _():
            pl.semaphore_signal(
                barrier, inc=1, device_id={"pairs": position + 2}, device_id_type=MESH
            )

        @pl.when(has_partner)
        def _():
            for far in range(1, count):
                pl.semaphore_signal(
                    barrier,
                    inc=1,
                    device_id={"rows": lax.rem(me + far, count), "pairs": partner},
                    device_id_type=MESH,
                )

        greeted = greeted + jnp.where(position >= 2, 1, 0) + jnp.where(position + 2 < length, 1, 0)
        greeted = greeted + jnp.where(has_partner, count - 1, 0)
    pl.semaphore_wait(barrier, greeted)

    if rotates:
        def turn(chunk, carry):
            load(chunk).wait()
            turned = dot_three(split(loaded[at(chunk), :]), (rot_high[...], rot_low[...]), 1)
            left, right = turned[:, :block], turned[:, block:]
            up[at(chunk), :] = jnp.where(lowest, right, left)
            other[at(chunk), :] = jnp.where(lowest, left, right)

            @pl.when(jnp.logical_not(highest))
            def _():
                to_upper(chunk).start()

            @pl.when(highest)
            def _():
                land_second[at(chunk), :] = left

            @pl.when(jnp.logical_not(lowest))
            def _():
                to_lower(chunk).start()

            @pl.when(lowest)
            def _():
                land_first[at(chunk), :] = left

            return carry

        if ahead and not sums:
            lax.fori_loop(0, LATE, turn, 0)

            @pl.when(jnp.logical_not(has_partner))
            def _():
                lax.fori_loop(LATE, CHUNKS, turn, 0)

            @pl.when(has_partner)
            def _():
                inner = pl.ds(pl.multiple_of(jnp.where(odd, block, 0), block), block)

                def turn_near(chunk, carry):
                    load(chunk).wait()
                    sent = dot_three(
                        split(loaded[at(chunk), :]), (rot_high[:, inner], rot_low[:, inner]), 1
                    )

                    @pl.when(odd)
                    def _():
                        other[at(chunk), :] = sent
                        to_lower(chunk).start()

                    @pl.when(even)
                    def _():
                        up[at(chunk), :] = sent
                        to_upper(chunk).start()

                    mine_block, far_block = had_kept[at(chunk), :], had_extra[at(chunk), :]
                    pair = jnp.concatenate(
                        [
                            jnp.where(odd, mine_block, far_block),
                            jnp.where(odd, far_block, mine_block),
                        ],
                        axis=1,
                    )
                    stays = dot_three(split(pair), (near_high[...], near_low[...]), 1)

                    @pl.when(odd)
                    def _():
                        land_second[at(chunk), :] = stays

                    @pl.when(even)
                    def _():
                        land_first[at(chunk), :] = stays

                    return carry

                for chunk in range(LATE, CHUNKS):
                    for copy in load_side(chunk):
                        copy.wait()
                lax.fori_loop(LATE, CHUNKS, turn_near, 0)

            @pl.when(jnp.logical_not(has_partner))
            def _():
                for chunk in range(LATE, CHUNKS):
                    for copy in load_side(chunk):
                        copy.wait()
        else:
            lax.fori_loop(0, CHUNKS, turn, 0)

        if ahead and sums:
            for chunk in range(LATE, CHUNKS):
                @pl.when(odd)
                def _():
                    keep(chunk, up).start()

                @pl.when(even)
                def _():
                    keep(chunk, other).start()

    if sums:
        cross[...] = jnp.zeros_like(cross)
        norms[...] = jnp.zeros_like(norms)

    def gets(chunk, edge, far_side):
        arrives = jnp.logical_not(edge)
        if ahead and not sums:
            own = jnp.logical_and(far_side, chunk >= LATE)
            arrives = jnp.logical_and(arrives, jnp.logical_not(own))
        return arrives

    def take(chunk, carry):
        if rotates:
            @pl.when(gets(chunk, lowest, even))
            def _():
                to_upper(chunk).wait_recv()

            @pl.when(gets(chunk, highest, odd))
            def _():
                to_lower(chunk).wait_recv()

            store(chunk, 0).start()
            store(chunk, 1).start()
        else:
            load(chunk).wait()
        if sums:
            if rotates:
                first, second = land_first[at(chunk), :], land_second[at(chunk), :]
            else:
                first, second = loaded[at(chunk), :block], loaded[at(chunk), block:]
            cross[...] += dot_three(split(first), split(second), 0)
            norms[0:1, :] += jnp.sum(first * first, axis=0, keepdims=True)
            norms[1:2, :] += jnp.sum(second * second, axis=0, keepdims=True)
        return carry

    lax.fori_loop(0, CHUNKS, take, 0)

    if sums:
        share = block // count
        half = block // 2
        for slot in range(count):
            part[slot, :share, :] = cross[slot * share : (slot + 1) * share, :half]
            part[slot, share : 2 * share, :] = cross[slot * share : (slot + 1) * share, half:]
            part[slot, 2 * share : 2 * share + 8, :] = norms[:, :half]
            part[slot, 2 * share + 8 : 2 * share + 16, :] = norms[:, half:]
        beside = None
        if ahead:
            beside = (partner, has_partner, total_near, gathered_near, send_near, recv_near)
        sum_over_rows(count, part, total, recv, mine, gathered, sums_sems, beside)
    if ahead and sums:
        @pl.when(jnp.logical_and(sends_extra, even))
        def _():
            for chunk in range(LATE, CHUNKS):
                to_extra(chunk, up, position + 2).start()

        @pl.when(jnp.logical_and(sends_extra, odd))
        def _():
            for chunk in range(LATE, CHUNKS):
                to_extra(chunk, other, position - 2).start()

        for chunk in range(LATE, CHUNKS):
            @pl.when(gets_extra)
            def _():
                to_extra(chunk, up, position).wait_recv()

            store_extra(chunk).start()
        for chunk in range(LATE, CHUNKS):
            @pl.when(sends_extra)
            def _():
                to_extra(chunk, up, position).wait_send()

            keep(chunk, up).wait()
            store_extra(chunk).wait()

    if rotates:
        def finish(chunk, carry):
            @pl.when(gets(chunk, highest, odd))
            def _():
                to_upper(chunk).wait_send()

            @pl.when(gets(chunk, lowest, even))
            def _():
                to_lower(chunk).wait_send()

            store(chunk, 0).wait()
            store(chunk, 1).wait()
            return carry

        lax.fori_loop(0, CHUNKS, finish, 0)


def stage(name, number, matrix, rotation, sums, ahead=False, side=()):
    rows, cols = matrix.shape
    block = cols // 2
    count = lax.axis_size("rows")
    length = lax.axis_size("pairs")
    rotates = rotation is not None
    slot = (2 * (block // count) + 16, block // 2)
    hbm = pl.BlockSpec(memory_space=pl.ANY)
    vmem = pl.BlockSpec(memory_space=pltpu.VMEM)
    dma = pltpu.SemaphoreType.DMA
    in_specs, outs, out_specs = [hbm], [], []
    scratch = [pltpu.VMEM((rows, cols), F32), dma((CHUNKS,))]
    if rotates:
        in_specs += [vmem, vmem]
        if side:
            in_specs += [hbm, hbm, vmem, vmem]
        outs.append(jax.ShapeDtypeStruct((rows, cols), F32))
        out_specs.append(hbm)
        scratch += [pltpu.VMEM((rows, block), F32)] * 4
        scratch += [dma((CHUNKS,))] * 4 + [dma((2, CHUNKS))]
    if sums:
        outs.append(jax.ShapeDtypeStruct((count,) + slot, F32))
        out_specs.append(vmem)
        if ahead:
            outs += [jax.ShapeDtypeStruct((rows, block), F32)] * 2 + [outs[-1]]
            out_specs += [hbm, hbm, vmem]
        scratch += [pltpu.VMEM((block, block), F32), pltpu.VMEM((8, block), F32)]
        scratch += [pltpu.VMEM((count,) + slot, F32)] * 2 + [pltpu.VMEM(slot, F32)]
        scratch += [pltpu.VMEM((count,) + slot, F32)]
        scratch += [dma((count,))] * 4
    if ahead and sums:
        scratch += [pltpu.VMEM((rows, block), F32), pltpu.VMEM((count,) + slot, F32)]
        scratch += [dma((CHUNKS,))] * 2 + [dma((count,))] * 2 + [dma((2, CHUNKS))]
    if ahead and not sums:
        scratch += [pltpu.VMEM((rows, block), F32)] * 2 + [dma((2, CHUNKS))]
    return pl.pallas_call(
        functools.partial(stage_kernel, rotates, sums, ahead, count, length),
        out_shape=outs,
        in_specs=in_specs,
        out_specs=out_specs,
        scratch_shapes=scratch,
        name=name,
        compiler_params=pltpu.CompilerParams(
            collective_id=number, has_side_effects=True, vmem_limit_bytes=50 * 2**20
        ),
    )(matrix, *(rotation or ()), *side)


def rotation_kernel(rows_all, problems, *refs):
    totals, refs = refs[:problems], refs[problems:]
    outs, (coupling, inverse, residual) = refs[: 2 * problems], refs[2 * problems :]
    count, depth, half = totals[0].shape
    block = 2 * half
    share = (depth - 16) // 2
    row = lax.broadcasted_iota(jnp.int32, (block, block), 0)
    col = lax.broadcasted_iota(jnp.int32, (block, block), 1)
    identity = jnp.where(row == col, 1.0, 0.0).astype(F32)

    def gram_of(turn):
        return lax.dot_general(
            turn,
            turn,
            (((1,), (1,)), ((), ())),
            precision=lax.Precision.HIGHEST,
            preferred_element_type=F32,
        )

    spread_most = None
    for index, total in enumerate(totals):
        for slot in range(count):
            rows = slice(slot * share, (slot + 1) * share)
            coupling[index, rows, :half] = total[slot, :share, :]
            coupling[index, rows, half:] = total[slot, share : 2 * share, :]
        norms = jnp.concatenate(
            [total[0, 2 * share : 2 * share + 8, :], total[0, 2 * share + 8 :, :]], axis=1
        )
        scales = lax.rsqrt(norms / rows_all + 1e-06)
        scale_first = jnp.sum(identity * scales[0:1, :], axis=1, keepdims=True)
        turn = 0.5 * coupling[index] * scale_first * scales[1:2, :] / rows_all
        coupling[index] = turn
        gram = gram_of(turn)
        spread = jnp.max(jnp.sum(jnp.abs(gram), axis=1, keepdims=True))
        start = 2.0 / (2.0 + spread)
        first = (1.0 - start) * identity - start * gram
        inverse[index] = start * (identity + first)
        residual[index] = exact_dot(first, first)
        spread_most = spread if index == 0 else jnp.maximum(spread_most, spread)
    bound = spread_most / (2.0 + spread_most)

    def grow(state):
        limit, trips = state
        for index in range(problems):
            both = exact_dot(
                jnp.concatenate([inverse[index], residual[index]], axis=0), residual[index]
            )
            inverse[index] += both[:block]
            residual[index] = both[block:]
        return limit * limit, trips + 1

    lax.while_loop(
        lambda state: jnp.logical_and(state[0] > 1e-07, state[1] < 30),
        grow,
        (bound * bound, jnp.int32(0)),
    )

    def correct(trip, carry):
        for index in range(problems):
            guess = inverse[index]
            residual[index] = identity - guess - exact_dot(gram_of(coupling[index]), guess)
            inverse[index] = guess + exact_dot(guess, residual[index])
        return carry

    lax.fori_loop(0, jnp.where(spread_most > 32.0, 4, 0), correct, 0)
    for index in range(problems):
        turn = coupling[index]
        upper = exact_dot(inverse[index], turn)
        lower = exact_dot(turn, upper, 0)
        left = (2.0 * inverse[index] - identity, -2.0 * upper.T)
        right = (2.0 * upper, identity - 2.0 * lower)
        for down in range(2):
            place = pl.ds(down * block, block)
            if index == 0:
                value = jnp.concatenate([left[down], right[down]], axis=1)
            else:
                odd = lax.rem(lax.axis_index("pairs"), 2) == 1
                value = jnp.where(odd, right[down], left[down])
            high, low = split(value)
            outs[2 * index][place, :] = high
            outs[2 * index + 1][place, :] = low


def rotation_of(rows_all, *totals):
    block = 2 * totals[0].shape[2]
    problems = len(totals)
    vmem = pl.BlockSpec(memory_space=pltpu.VMEM)
    outs = [jax.ShapeDtypeStruct((2 * block, 2 * block), BF16)] * 2
    if problems > 1:
        outs += [jax.ShapeDtypeStruct((2 * block, block), BF16)] * 2
    return pl.pallas_call(
        functools.partial(rotation_kernel, rows_all, problems),
        out_shape=outs,
        in_specs=[vmem] * problems,
        out_specs=[vmem] * len(outs),
        scratch_shapes=[pltpu.VMEM((problems, block, block), F32)] * 3,
        name="rotation",
        compiler_params=pltpu.CompilerParams(vmem_limit_bytes=32 * 2**20),
    )(*totals)


def shards(matrix):
    rows_all = matrix.shape[0] * lax.axis_size("rows")
    (total,) = stage("products", 0, matrix, None, True)
    rotation = rotation_of(rows_all, total)
    matrix, total, kept, extra, total_near = stage(
        "turn_and_products", 1, matrix, rotation, True, True
    )
    high, low, near_high, near_low = rotation_of(rows_all, total, total_near)
    (matrix,) = stage(
        "last_turn", 2, matrix, (high, low), False, True, (kept, extra, near_high, near_low)
    )
    return matrix


def solution(mesh):
    return jax.shard_map(
        shards,
        mesh=mesh,
        in_specs=(P("rows", "pairs"),),
        out_specs=P("rows", "pairs"),
        check_vma=False,
    )
```

```python
import functools

import jax
import jax.numpy as jnp
from jax import lax
from jax.experimental import pallas as pl
from jax.experimental.pallas import tpu as pltpu
from jax.sharding import PartitionSpec as P

CHUNKS = 8
LATE = 3
F32 = jnp.float32
BF16 = jnp.bfloat16
MESH = pl.DeviceIdType.MESH


def split(value):
    high = value.astype(BF16)
    return high, (value - high.astype(F32)).astype(BF16)


def dot_bf16(left, right, left_dim):
    return lax.dot_general(
        left, right, (((left_dim,), (0,)), ((), ())), preferred_element_type=F32
    )


def dot_three(left, right, left_dim):
    return (
        dot_bf16(left[0], right[1], left_dim)
        + dot_bf16(left[1], right[0], left_dim)
        + dot_bf16(left[0], right[0], left_dim)
    )


def exact_dot(left, right, left_dim=1):
    return lax.dot_general(
        left,
        right,
        (((left_dim,), (0,)), ((), ())),
        precision=lax.Precision.HIGHEST,
        preferred_element_type=F32,
    )


def sum_over_rows(count, part, total, recv, mine, gathered, sems, beside):
    send_one, recv_one, send_two, recv_two = sems
    me = lax.axis_index("rows")
    first_copies = []
    for far in range(1, count):
        peer = lax.rem(me + far, count)
        copy = pltpu.make_async_remote_copy(
            src_ref=part.at[peer],
            dst_ref=recv.at[far],
            send_sem=send_one.at[far],
            recv_sem=recv_one.at[far],
            device_id={"rows": peer},
            device_id_type=MESH,
        )
        copy.start()
        first_copies.append(copy)
    acc = part[me]
    for far in range(1, count):
        first_copies[far - 1].wait_recv()
        acc = acc + recv[far]
    mine[...] = acc
    second_copies = []
    for far in range(1, count):
        peer = lax.rem(me + far, count)
        copy = pltpu.make_async_remote_copy(
            src_ref=mine,
            dst_ref=gathered.at[far],
            send_sem=send_two.at[far],
            recv_sem=recv_two.at[far],
            device_id={"rows": peer},
            device_id_type=MESH,
        )
        copy.start()
        second_copies.append(copy)
    if beside:
        partner, has_partner, total_near, gathered_near, send_near, recv_near = beside

        def to_near(far):
            return pltpu.make_async_remote_copy(
                src_ref=mine,
                dst_ref=gathered_near.at[far],
                send_sem=send_near.at[far],
                recv_sem=recv_near.at[far],
                device_id={"rows": lax.rem(me + far, count), "pairs": partner},
                device_id_type=MESH,
            )

        @pl.when(has_partner)
        def _():
            for far in range(count):
                to_near(far).start()

    total[me] = acc
    for far in range(1, count):
        second_copies[far - 1].wait_recv()
        total[lax.rem(me + count - far, count)] = gathered[far]
    if beside:
        @pl.when(has_partner)
        def _():
            for far in range(count):
                to_near(far).wait_recv()
                total_near[lax.rem(me + count - far, count)] = gathered_near[far]
            for far in range(count):
                to_near(far).wait_send()

        @pl.when(jnp.logical_not(has_partner))
        def _():
            total_near[...] = total[...]

    for copy in first_copies + second_copies:
        copy.wait_send()


def stage_kernel(rotates, sums, ahead, count, length, *refs):
    refs = list(refs)
    matrix = refs.pop(0)
    if rotates:
        rot_high, rot_low = refs.pop(0), refs.pop(0)
        if ahead and not sums:
            kept, extra, near_high, near_low = (refs.pop(0) for _ in range(4))
        moved = refs.pop(0)
    if sums:
        total = refs.pop(0)
        if ahead:
            kept, extra, total_near = (refs.pop(0) for _ in range(3))
    loaded, load_sem = refs.pop(0), refs.pop(0)
    if rotates:
        up, other, land_first, land_second = (refs.pop(0) for _ in range(4))
        up_send, up_recv, down_send, down_recv, store_sem = (refs.pop(0) for _ in range(5))
    if sums:
        cross, norms, part, recv, mine, gathered = (refs.pop(0) for _ in range(6))
        sums_sems = tuple(refs.pop(0) for _ in range(4))
    if ahead and sums:
        land_extra, gathered_near = refs.pop(0), refs.pop(0)
        extra_send, extra_recv, send_near, recv_near, side_sem = (refs.pop(0) for _ in range(5))
    if ahead and not sums:
        had_kept, had_extra, side_sem = (refs.pop(0) for _ in range(3))
    rows, cols = loaded.shape
    block = cols // 2
    step = rows // CHUNKS
    position = lax.axis_index("pairs")
    lowest = position == 0
    highest = position == length - 1
    odd = lax.rem(position, 2) == 1
    even = jnp.logical_not(odd)
    has_partner = jnp.logical_or(
        jnp.logical_and(odd, position < length - 1), jnp.logical_and(even, position > 0)
    )
    sends_extra = jnp.logical_or(
        jnp.logical_and(even, position + 2 < length), jnp.logical_and(odd, position >= 2)
    )
    gets_extra = jnp.logical_or(
        jnp.logical_and(even, position >= 2), jnp.logical_and(odd, position + 2 < length)
    )
    partner = lax.rem(position + jnp.where(odd, 1, length - 1), length)

    def at(chunk):
        return pl.ds(pl.multiple_of(chunk * step, step), step)

    def load(chunk):
        return pltpu.make_async_copy(
            matrix.at[at(chunk)], loaded.at[at(chunk)], load_sem.at[chunk]
        )

    def to_upper(chunk):
        return pltpu.make_async_remote_copy(
            src_ref=up.at[at(chunk)],
            dst_ref=land_first.at[at(chunk)],
            send_sem=up_send.at[chunk],
            recv_sem=up_recv.at[chunk],
            device_id={"pairs": lax.rem(position + 1, length)},
            device_id_type=MESH,
        )

    def to_lower(chunk):
        return pltpu.make_async_remote_copy(
            src_ref=other.at[at(chunk)],
            dst_ref=land_second.at[at(chunk)],
            send_sem=down_send.at[chunk],
            recv_sem=down_recv.at[chunk],
            device_id={"pairs": lax.rem(position + length - 1, length)},
            device_id_type=MESH,
        )

    def store(chunk, half):
        source = land_second if half else land_first
        return pltpu.make_async_copy(
            source.at[at(chunk)],
            moved.at[at(chunk), pl.ds(half * block, block)],
            store_sem.at[half, chunk],
        )

    def to_extra(chunk, source, target):
        return pltpu.make_async_remote_copy(
            src_ref=source.at[at(chunk)],
            dst_ref=land_extra.at[at(chunk)],
            send_sem=extra_send.at[chunk],
            recv_sem=extra_recv.at[chunk],
            device_id={"pairs": lax.rem(target + length, length)},
            device_id_type=MESH,
        )

    def keep(chunk, source):
        return pltpu.make_async_copy(source.at[at(chunk)], kept.at[at(chunk)], side_sem.at[0, chunk])

    def store_extra(chunk):
        return pltpu.make_async_copy(
            land_extra.at[at(chunk)], extra.at[at(chunk)], side_sem.at[1, chunk]
        )

    def load_side(chunk):
        return (
            pltpu.make_async_copy(kept.at[at(chunk)], had_kept.at[at(chunk)], side_sem.at[0, chunk]),
            pltpu.make_async_copy(extra.at[at(chunk)], had_extra.at[at(chunk)], side_sem.at[1, chunk]),
        )

    for chunk in range(CHUNKS):
        load(chunk).start()
        if ahead and not sums and chunk >= LATE:
            for copy in load_side(chunk):
                copy.start()

    barrier = pltpu.get_barrier_semaphore()
    if sums:
        me = lax.axis_index("rows")
        for far in range(1, count):
            pl.semaphore_signal(
                barrier,
                inc=1,
                device_id={"rows": lax.rem(me + far, count)},
                device_id_type=MESH,
            )
    greeted = jnp.int32(count - 1 if sums else 0)
    if rotates:
        @pl.when(jnp.logical_not(lowest))
        def _():
            pl.semaphore_signal(
                barrier, inc=1, device_id={"pairs": position - 1}, device_id_type=MESH
            )

        @pl.when(jnp.logical_not(highest))
        def _():
            pl.semaphore_signal(
                barrier, inc=1, device_id={"pairs": position + 1}, device_id_type=MESH
            )

        greeted = greeted + jnp.where(lowest, 0, 1) + jnp.where(highest, 0, 1)
    if ahead and sums:
        @pl.when(position >= 2)
        def _():
            pl.semaphore_signal(
                barrier, inc=1, device_id={"pairs": position - 2}, device_id_type=MESH
            )

        @pl.when(position + 2 < length)
        def _():
            pl.semaphore_signal(
                barrier, inc=1, device_id={"pairs": position + 2}, device_id_type=MESH
            )

        @pl.when(has_partner)
        def _():
            for far in range(1, count):
                pl.semaphore_signal(
                    barrier,
                    inc=1,
                    device_id={"rows": lax.rem(me + far, count), "pairs": partner},
                    device_id_type=MESH,
                )

        greeted = greeted + jnp.where(position >= 2, 1, 0) + jnp.where(position + 2 < length, 1, 0)
        greeted = greeted + jnp.where(has_partner, count - 1, 0)
    pl.semaphore_wait(barrier, greeted)

    if rotates:
        def turn(chunk, carry):
            load(chunk).wait()
            turned = dot_three(split(loaded[at(chunk), :]), (rot_high[...], rot_low[...]), 1)
            left, right = turned[:, :block], turned[:, block:]
            up[at(chunk), :] = jnp.where(lowest, right, left)
            other[at(chunk), :] = jnp.where(lowest, left, right)

            @pl.when(jnp.logical_not(highest))
            def _():
                to_upper(chunk).start()

            @pl.when(highest)
            def _():
                land_second[at(chunk), :] = left

            @pl.when(jnp.logical_not(lowest))
            def _():
                to_lower(chunk).start()

            @pl.when(lowest)
            def _():
                land_first[at(chunk), :] = left

            return carry

        if ahead and not sums:
            lax.fori_loop(0, LATE, turn, 0)

            @pl.when(jnp.logical_not(has_partner))
            def _():
                lax.fori_loop(LATE, CHUNKS, turn, 0)

            @pl.when(has_partner)
            def _():
                inner = pl.ds(pl.multiple_of(jnp.where(odd, block, 0), block), block)

                def turn_near(chunk, carry):
                    load(chunk).wait()
                    sent = dot_three(
                        split(loaded[at(chunk), :]), (rot_high[:, inner], rot_low[:, inner]), 1
                    )

                    @pl.when(odd)
                    def _():
                        other[at(chunk), :] = sent
                        to_lower(chunk).start()

                    @pl.when(even)
                    def _():
                        up[at(chunk), :] = sent
                        to_upper(chunk).start()

                    mine_block, far_block = had_kept[at(chunk), :], had_extra[at(chunk), :]
                    pair = jnp.concatenate(
                        [
                            jnp.where(odd, mine_block, far_block),
                            jnp.where(odd, far_block, mine_block),
                        ],
                        axis=1,
                    )
                    stays = dot_three(split(pair), (near_high[...], near_low[...]), 1)

                    @pl.when(odd)
                    def _():
                        land_second[at(chunk), :] = stays

                    @pl.when(even)
                    def _():
                        land_first[at(chunk), :] = stays

                    return carry

                for chunk in range(LATE, CHUNKS):
                    for copy in load_side(chunk):
                        copy.wait()
                lax.fori_loop(LATE, CHUNKS, turn_near, 0)

            @pl.when(jnp.logical_not(has_partner))
            def _():
                for chunk in range(LATE, CHUNKS):
                    for copy in load_side(chunk):
                        copy.wait()
        else:
            lax.fori_loop(0, CHUNKS, turn, 0)

        if ahead and sums:
            for chunk in range(LATE, CHUNKS):
                @pl.when(odd)
                def _():
                    keep(chunk, up).start()

                @pl.when(even)
                def _():
                    keep(chunk, other).start()

    if sums:
        cross[...] = jnp.zeros_like(cross)
        norms[...] = jnp.zeros_like(norms)

    def gets(chunk, edge, far_side):
        arrives = jnp.logical_not(edge)
        if ahead and not sums:
            own = jnp.logical_and(far_side, chunk >= LATE)
            arrives = jnp.logical_and(arrives, jnp.logical_not(own))
        return arrives

    def take(chunk, carry):
        if rotates:
            @pl.when(gets(chunk, lowest, even))
            def _():
                to_upper(chunk).wait_recv()

            @pl.when(gets(chunk, highest, odd))
            def _():
                to_lower(chunk).wait_recv()

            store(chunk, 0).start()
            store(chunk, 1).start()
        else:
            load(chunk).wait()
        if sums:
            if rotates:
                first, second = land_first[at(chunk), :], land_second[at(chunk), :]
            else:
                first, second = loaded[at(chunk), :block], loaded[at(chunk), block:]
            cross[...] += dot_three(split(first), split(second), 0)
            norms[0:1, :] += jnp.sum(first * first, axis=0, keepdims=True)
            norms[1:2, :] += jnp.sum(second * second, axis=0, keepdims=True)
        return carry

    lax.fori_loop(0, CHUNKS, take, 0)

    if sums:
        share = block // count
        half = block // 2
        for slot in range(count):
            part[slot, :share, :] = cross[slot * share : (slot + 1) * share, :half]
            part[slot, share : 2 * share, :] = cross[slot * share : (slot + 1) * share, half:]
            part[slot, 2 * share : 2 * share + 8, :] = norms[:, :half]
            part[slot, 2 * share + 8 : 2 * share + 16, :] = norms[:, half:]
        beside = None
        if ahead:
            beside = (partner, has_partner, total_near, gathered_near, send_near, recv_near)
        sum_over_rows(count, part, total, recv, mine, gathered, sums_sems, beside)
    if ahead and sums:
        @pl.when(jnp.logical_and(sends_extra, even))
        def _():
            for chunk in range(LATE, CHUNKS):
                to_extra(chunk, up, position + 2).start()

        @pl.when(jnp.logical_and(sends_extra, odd))
        def _():
            for chunk in range(LATE, CHUNKS):
                to_extra(chunk, other, position - 2).start()

        for chunk in range(LATE, CHUNKS):
            @pl.when(gets_extra)
            def _():
                to_extra(chunk, up, position).wait_recv()

            store_extra(chunk).start()
        for chunk in range(LATE, CHUNKS):
            @pl.when(sends_extra)
            def _():
                to_extra(chunk, up, position).wait_send()

            keep(chunk, up).wait()
            store_extra(chunk).wait()

    if rotates:
        def finish(chunk, carry):
            @pl.when(gets(chunk, highest, odd))
            def _():
                to_upper(chunk).wait_send()

            @pl.when(gets(chunk, lowest, even))
            def _():
                to_lower(chunk).wait_send()

            store(chunk, 0).wait()
            store(chunk, 1).wait()
            return carry

        lax.fori_loop(0, CHUNKS, finish, 0)


def stage(name, number, matrix, rotation, sums, ahead=False, side=()):
    rows, cols = matrix.shape
    block = cols // 2
    count = lax.axis_size("rows")
    length = lax.axis_size("pairs")
    rotates = rotation is not None
    slot = (2 * (block // count) + 16, block // 2)
    hbm = pl.BlockSpec(memory_space=pl.ANY)
    vmem = pl.BlockSpec(memory_space=pltpu.VMEM)
    dma = pltpu.SemaphoreType.DMA
    in_specs, outs, out_specs = [hbm], [], []
    scratch = [pltpu.VMEM((rows, cols), F32), dma((CHUNKS,))]
    if rotates:
        in_specs += [vmem, vmem]
        if side:
            in_specs += [hbm, hbm, vmem, vmem]
        outs.append(jax.ShapeDtypeStruct((rows, cols), F32))
        out_specs.append(hbm)
        scratch += [pltpu.VMEM((rows, block), F32)] * 4
        scratch += [dma((CHUNKS,))] * 4 + [dma((2, CHUNKS))]
    if sums:
        outs.append(jax.ShapeDtypeStruct((count,) + slot, F32))
        out_specs.append(vmem)
        if ahead:
            outs += [jax.ShapeDtypeStruct((rows, block), F32)] * 2 + [outs[-1]]
            out_specs += [hbm, hbm, vmem]
        scratch += [pltpu.VMEM((block, block), F32), pltpu.VMEM((8, block), F32)]
        scratch += [pltpu.VMEM((count,) + slot, F32)] * 2 + [pltpu.VMEM(slot, F32)]
        scratch += [pltpu.VMEM((count,) + slot, F32)]
        scratch += [dma((count,))] * 4
    if ahead and sums:
        scratch += [pltpu.VMEM((rows, block), F32), pltpu.VMEM((count,) + slot, F32)]
        scratch += [dma((CHUNKS,))] * 2 + [dma((count,))] * 2 + [dma((2, CHUNKS))]
    if ahead and not sums:
        scratch += [pltpu.VMEM((rows, block), F32)] * 2 + [dma((2, CHUNKS))]
    return pl.pallas_call(
        functools.partial(stage_kernel, rotates, sums, ahead, count, length),
        out_shape=outs,
        in_specs=in_specs,
        out_specs=out_specs,
        scratch_shapes=scratch,
        name=name,
        compiler_params=pltpu.CompilerParams(
            collective_id=number, has_side_effects=True, vmem_limit_bytes=50 * 2**20
        ),
    )(matrix, *(rotation or ()), *side)


def rotation_kernel(rows_all, problems, *refs):
    totals, refs = refs[:problems], refs[problems:]
    outs, (coupling, inverse, residual) = refs[: 2 * problems], refs[2 * problems :]
    count, depth, half = totals[0].shape
    block = 2 * half
    share = (depth - 16) // 2
    row = lax.broadcasted_iota(jnp.int32, (block, block), 0)
    col = lax.broadcasted_iota(jnp.int32, (block, block), 1)
    identity = jnp.where(row == col, 1.0, 0.0).astype(F32)

    def gram_of(turn):
        return lax.dot_general(
            turn,
            turn,
            (((1,), (1,)), ((), ())),
            precision=lax.Precision.HIGHEST,
            preferred_element_type=F32,
        )

    spread_most = None
    for index, total in enumerate(totals):
        for slot in range(count):
            rows = slice(slot * share, (slot + 1) * share)
            coupling[index, rows, :half] = total[slot, :share, :]
            coupling[index, rows, half:] = total[slot, share : 2 * share, :]
        norms = jnp.concatenate(
            [total[0, 2 * share : 2 * share + 8, :], total[0, 2 * share + 8 :, :]], axis=1
        )
        scales = lax.rsqrt(norms / rows_all + 1e-06)
        scale_first = jnp.sum(identity * scales[0:1, :], axis=1, keepdims=True)
        turn = 0.5 * coupling[index] * scale_first * scales[1:2, :] / rows_all
        coupling[index] = turn
        gram = gram_of(turn)
        spread = jnp.max(jnp.sum(jnp.abs(gram), axis=1, keepdims=True))
        start = 2.0 / (2.0 + spread)
        first = (1.0 - start) * identity - start * gram
        inverse[index] = start * (identity + first)
        parts = split(first)
        residual[index] = dot_three(parts, parts, 1)
        spread_most = spread if index == 0 else jnp.maximum(spread_most, spread)
    bound = spread_most / (2.0 + spread_most)

    def grow(state):
        limit, trips = state
        for index in range(problems):
            high, low = split(residual[index])
            inverse_high, inverse_low = split(inverse[index])
            both = dot_three(
                (
                    jnp.concatenate([inverse_high, high], axis=0),
                    jnp.concatenate([inverse_low, low], axis=0),
                ),
                (high, low),
                1,
            )
            inverse[index] += both[:block]
            residual[index] = both[block:]
        return limit * limit, trips + 1

    lax.while_loop(
        lambda state: jnp.logical_and(state[0] > 1e-07, state[1] < 30),
        grow,
        (bound * bound, jnp.int32(0)),
    )

    def correct(trip, carry):
        for index in range(problems):
            guess = inverse[index]
            residual[index] = identity - guess - exact_dot(gram_of(coupling[index]), guess)
            inverse[index] = guess + exact_dot(guess, residual[index])
        return carry

    lax.fori_loop(0, jnp.where(spread_most > 32.0, 4, 0), correct, 0)
    for index in range(problems):
        turn = coupling[index]
        upper = exact_dot(inverse[index], turn)
        lower = exact_dot(turn, upper, 0)
        left = (2.0 * inverse[index] - identity, -2.0 * upper.T)
        right = (2.0 * upper, identity - 2.0 * lower)
        for down in range(2):
            place = pl.ds(down * block, block)
            if index == 0:
                value = jnp.concatenate([left[down], right[down]], axis=1)
            else:
                odd = lax.rem(lax.axis_index("pairs"), 2) == 1
                value = jnp.where(odd, right[down], left[down])
            high, low = split(value)
            outs[2 * index][place, :] = high
            outs[2 * index + 1][place, :] = low


def rotation_of(rows_all, *totals):
    block = 2 * totals[0].shape[2]
    problems = len(totals)
    vmem = pl.BlockSpec(memory_space=pltpu.VMEM)
    outs = [jax.ShapeDtypeStruct((2 * block, 2 * block), BF16)] * 2
    if problems > 1:
        outs += [jax.ShapeDtypeStruct((2 * block, block), BF16)] * 2
    return pl.pallas_call(
        functools.partial(rotation_kernel, rows_all, problems),
        out_shape=outs,
        in_specs=[vmem] * problems,
        out_specs=[vmem] * len(outs),
        scratch_shapes=[pltpu.VMEM((problems, block, block), F32)] * 3,
        name="rotation",
        compiler_params=pltpu.CompilerParams(vmem_limit_bytes=32 * 2**20),
    )(*totals)


def copy_kernel(source, target):
    target[...] = source[...]


def written(matrix):
    rows, cols = matrix.shape
    spec = pl.BlockSpec((rows // CHUNKS, cols), lambda chunk: (chunk, 0))
    return pl.pallas_call(
        copy_kernel,
        out_shape=jax.ShapeDtypeStruct(matrix.shape, matrix.dtype),
        grid=(CHUNKS,),
        in_specs=[spec],
        out_specs=spec,
        name="written",
    )(matrix)


def shards(matrix):
    rows_all = matrix.shape[0] * lax.axis_size("rows")
    (total,) = stage("products", 0, matrix, None, True)
    rotation = rotation_of(rows_all, total)
    matrix, total, kept, extra, total_near = stage(
        "turn_and_products", 1, matrix, rotation, True, True
    )
    high, low, near_high, near_low = rotation_of(rows_all, total, total_near)
    (matrix,) = stage(
        "last_turn", 2, matrix, (high, low), False, True, (kept, extra, near_high, near_low)
    )
    return written(matrix)


def solution(mesh):
    return jax.shard_map(
        shards,
        mesh=mesh,
        in_specs=(P("rows", "pairs"),),
        out_specs=P("rows", "pairs"),
        check_vma=False,
    )
```
